128 devices in a mesh: dom: 16 (over x, y), sub: 8 (over z, core).
Axes of the slice: x: 4, y: 4, z: 4, core: 2. Of those that a mesh axis runs over, the one named last changes fastest.
Arguments:
- features: bfloat16 [131072, 602], P(('dom', 'sub')), may hold values from -6 to 6
- w_inner: bfloat16 [602, 256], replicated, may hold values from -0.25 to 0.25
- bias_inner: float32 [256], replicated, may hold values from -6 to 6
- w_outer: bfloat16 [256, 41], replicated, may hold values from -0.375 to 0.375
- bias_outer: float32 [41], replicated, may hold values from -6 to 6
- tiles: bfloat16 [1024, 32, 128, 128], P(('dom', 'sub')), may hold values from -3 to 3
- tile_col: int32 [1024, 32], P(('dom', 'sub')), may hold values from 0 to 135, as said below
- degrees: int32 [131072], P(('dom', 'sub')), may hold values from 1 to 32
- send_rows: int32 [128, 128, 128], P(('dom', 'sub')), may hold values from -1 to 1023, as said below
Outputs:
- logits: float32 [131072, 41], P(('dom', 'sub'))
The draws below stay inside these ranges and needn't reach their ends.
Inputs may be any that keep to these rules, and one draw needn't show every extreme that they name: send_rows[e, p, s] is the row, among device e's 1024 vertices, that fills slot s of e's list for device p, or -1 for an unused slot; live slots come first and every list has 1 to 128 live slots; every sender has a full list, and in every draw some device receives full lists from all senders. tile_col[d * 8 + r, t] is the column block, in device d's column space, of tile t of row block r; the 32 column blocks of a row block are distinct.
All inputs are finite; a program needn't handle non-finite values.
Results may differ from the reference program's by a relative error of at most 0.0042.
Values may be sent and summed in bfloat16 or wider, within the bound.
A program may use at most 128 MiB of HBM per device.

```python
import jax
import jax.numpy as jnp
from jax import lax

F_IN = 602
HID = 256
CLASSES = 41
BLK = 128
TILES = 32
V_DEV = 1024
PEERS = 128
ROW_BLOCKS = 8
COL_BLOCKS = 136
VERTS = 131072


def draw_send_rows(key, part):
    key_rows = jax.random.fold_in(key, 11)
    key_counts = jax.random.fold_in(key, 12)
    key_full = jax.random.fold_in(key, 13)
    key_target = jax.random.fold_in(key, 14)
    picked = jax.random.randint(key_rows, (PEERS, PEERS, BLK), 0, V_DEV)
    counts = jax.random.randint(key_counts, (PEERS, PEERS), 1, BLK + 1)
    full_peer = jax.random.randint(key_full, (PEERS,), 0, PEERS)
    target = jax.random.randint(key_target, (), 0, PEERS)
    peer_ids = jnp.arange(PEERS)
    counts = jnp.where(peer_ids[None, :] == full_peer[:, None], BLK, counts)
    counts = jnp.where(peer_ids[None, :] == target, BLK, counts)
    slots = jnp.arange(BLK)
    return jnp.where(slots[None, None, :] < counts[:, :, None], picked, -1).astype(jnp.int32)


def draw_tile_col(key, part):
    keys = jax.random.split(jax.random.fold_in(key, 21), PEERS)
    orders = jax.vmap(lambda single: jax.random.permutation(single, COL_BLOCKS))(keys)
    flat = jnp.arange(ROW_BLOCKS * TILES) % COL_BLOCKS
    picked = orders[:, flat]
    return picked.reshape(PEERS * ROW_BLOCKS, TILES).astype(jnp.int32)


def place_ends(drawn, stream_key, least, top_value):
    index_at = [jax.random.randint(jax.random.fold_in(stream_key, axis), (), 0, length) for axis, length in enumerate(drawn.shape)]
    main_axis = drawn.shape.index(max(drawn.shape))
    beside = index_at[:main_axis] + [(index_at[main_axis] + 1) % drawn.shape[main_axis]] + index_at[main_axis + 1:]
    return drawn.at[tuple(index_at)].set(least).at[tuple(beside)].set(top_value)


def levels(rng, dims, shards, low, largest):
    def one(position, blocks):
        draws = jax.random.uniform(jax.random.fold_in(jax.random.fold_in(rng, 6), position), (blocks,), jnp.float32, low / len(shards), largest / len(shards))
        return jnp.repeat(jnp.exp(draws), dims[position] // blocks).reshape((-1,) + (1,) * (len(dims) - position - 1))

    gain = one(*shards[0])
    for cut in shards[1:]:
        gain = gain * one(*cut)
    return gain


def centred(stream_key, extent, scale, reach, cuts=(), kind=jnp.bfloat16):
    drawn = scale * jax.random.normal(stream_key, extent, jnp.float32)
    if cuts:
        drawn = drawn * levels(stream_key, extent, cuts, -0.22, 0.18)
    return jnp.clip(drawn, -reach, reach).astype(kind)


def setup_inputs(seed: int = 0) -> dict:
    key_of = jax.random.split(jax.random.key(seed), 10)
    return {
        "features": centred(key_of[0], (VERTS, F_IN), 1.0, 6.0, ((0, 128),)),
        "w_inner": centred(key_of[1], (F_IN, HID), F_IN ** -0.5, 0.25),
        "bias_inner": centred(key_of[2], (HID,), 1.0, 6.0, (), jnp.float32),
        "w_outer": centred(key_of[3], (HID, CLASSES), HID ** -0.5, 0.375),
        "bias_outer": centred(key_of[4], (CLASSES,), 1.0, 6.0, (), jnp.float32),
        "tiles": centred(key_of[5], (PEERS * ROW_BLOCKS, TILES, BLK, BLK), (12.0 / (TILES * BLK) ** 0.5), 3.0, ((0, 128),)),
        "tile_col": draw_tile_col(jax.random.fold_in(key_of[9], 71), 0),
        "degrees": place_ends(jax.random.randint(key_of[7], (VERTS,), 1, 33), jax.random.fold_in(key_of[7], 1), 1, 32).astype(jnp.int32),
        "send_rows": draw_send_rows(jax.random.fold_in(key_of[9], 71), 0),
    }


def aggregate(feature_rows, tiles, tile_col, send_rows):
    width = feature_rows.shape[1]
    by_device = feature_rows.reshape(PEERS, V_DEV, width)
    tile_sets = tiles.reshape(PEERS, ROW_BLOCKS, TILES, BLK, BLK)
    col_sets = tile_col.reshape(PEERS, ROW_BLOCKS, TILES)

    def per_target(target):
        slot_rows = lax.dynamic_index_in_dim(send_rows, target, 1, keepdims=False)
        clipped = jnp.clip(slot_rows, 0, V_DEV - 1).astype(jnp.int32)
        fetched = jnp.take_along_axis(by_device, clipped[:, :, None], axis=1)
        fetched = jnp.where((slot_rows >= 0)[:, :, None], fetched, jnp.zeros((), feature_rows.dtype))
        own_rows = lax.dynamic_index_in_dim(by_device, target, 0, keepdims=False)
        columns = jnp.concatenate([own_rows.reshape(ROW_BLOCKS, BLK, width), fetched], axis=0)
        target_tiles = lax.dynamic_index_in_dim(tile_sets, target, 0, keepdims=False)
        target_cols = lax.dynamic_index_in_dim(col_sets, target, 0, keepdims=False)
        blocks = columns[target_cols]
        summed = jnp.einsum('rtij,rtjw->riw', target_tiles.astype(jnp.float32), blocks.astype(jnp.float32))
        return summed.reshape(V_DEV, width)
    results = lax.map(per_target, jnp.arange(PEERS, dtype=jnp.int32))
    return results.reshape(PEERS * V_DEV, width)

def reference(features, w_inner, bias_inner, w_outer, bias_outer, tiles, tile_col, degrees, send_rows):
    inv_sqrt = lax.rsqrt(degrees.astype(jnp.float32))[:, None]
    projected = (jnp.dot(features, w_inner, preferred_element_type=jnp.float32) * inv_sqrt).astype(jnp.bfloat16)
    agg_inner = aggregate(projected, tiles, tile_col, send_rows)
    hidden = (inv_sqrt * jax.nn.relu(inv_sqrt * agg_inner + bias_inner)).astype(jnp.bfloat16)
    scores = jnp.dot(hidden, w_outer, preferred_element_type=jnp.float32).astype(jnp.bfloat16)
    agg_outer = aggregate(scores, tiles, tile_col, send_rows)
    return inv_sqrt * agg_outer + bias_outer
```

```python
import functools

import jax
import jax.numpy as jnp
from jax import lax
from jax.experimental import pallas as pl
from jax.experimental.pallas import tpu as pltpu
from jax.sharding import PartitionSpec as P

BLOCK = 128
CHUNK = 256
LISTS = 8


def pick_rows(stacked, lists, width):
    parts = stacked.shape[0] // width
    index = jnp.concatenate([lists[0:1], lists[1:2]], axis=1)
    low = jnp.where(index >= 0, lax.rem(index, CHUNK), -1)
    high = lax.shift_right_arithmetic(index, 8)
    lane = lax.broadcasted_iota(jnp.int32, (CHUNK, 2 * BLOCK), 0)
    onehot = jnp.where(lane == low, 1.0, 0.0).astype(jnp.bfloat16)
    found = jnp.dot(stacked, onehot, preferred_element_type=jnp.float32)
    total = jnp.zeros((width, 2 * BLOCK), jnp.float32)
    for part in range(parts):
        total = jnp.where(high == part, found[part * width : (part + 1) * width], total)
    return total.astype(jnp.bfloat16)


def fill_lists(stacked, send_ref, out_ref, width):
    for pair in range(LISTS // 2):
        picked = pick_rows(stacked[...], send_ref[2 * pair : 2 * pair + 2, :], width)
        out_ref[2 * pair] = picked[:, :BLOCK]
        out_ref[2 * pair + 1] = picked[:, BLOCK:]


def project_kernel(features, w_inner, degrees, send, lists, local, stacked):
    width = w_inner.shape[1]

    @pl.when(pl.program_id(0) == 0)
    def _():
        inv_sqrt = lax.rsqrt(degrees[...].astype(jnp.float32))
        for part in range(stacked.shape[0] // width):
            rows = slice(part * CHUNK, (part + 1) * CHUNK)
            product = lax.dot_general(
                w_inner[...],
                features[rows, :],
                (((0,), (1,)), ((), ())),
                preferred_element_type=jnp.float32,
            )
            piece = (product * inv_sqrt[:, rows]).astype(jnp.bfloat16)
            stacked[part * width : (part + 1) * width, :] = piece
            local[2 * part] = piece[:, :BLOCK]
            local[2 * part + 1] = piece[:, BLOCK:]

    fill_lists(stacked, send, lists, width)


def gather_kernel(scores, send, lists, stacked):
    width = scores.shape[1]

    @pl.when(pl.program_id(0) == 0)
    def _():
        for block in range(scores.shape[0]):
            part, half = block // 2, block % 2
            stacked[part * width : (part + 1) * width, half * BLOCK : (half + 1) * BLOCK] = scores[block]

    fill_lists(stacked, send, lists, width)


def summed(tile_col, tiles, columns, row):
    total = None
    for pair in range(tiles.shape[1] // 2):
        first, second = tile_col[row, 2 * pair], tile_col[row, 2 * pair + 1]
        rows = jnp.concatenate([columns[first], columns[second]], axis=1)
        edges = jnp.concatenate([tiles[0, 2 * pair], tiles[0, 2 * pair + 1]], axis=1)
        product = lax.dot_general(
            rows, edges, (((1,), (1,)), ((), ())), preferred_element_type=jnp.float32
        )
        total = product if total is None else total + product
    return total


def load_columns(local, arrived, columns, sems):
    @pl.when(pl.program_id(0) == 0)
    def _():
        own = local.shape[0]
        first = pltpu.make_async_copy(local, columns.at[pl.ds(0, own)], sems.at[0])
        second = pltpu.make_async_copy(arrived, columns.at[pl.ds(own, arrived.shape[0])], sems.at[1])
        first.start()
        second.start()
        first.wait()
        second.wait()


def inner_kernel(tile_col, tiles, local, arrived, degrees, bias, w_outer, scores, columns, sems):
    load_columns(local, arrived, columns, sems)
    inv_sqrt = lax.rsqrt(degrees[...].astype(jnp.float32))
    aggregated = summed(tile_col, tiles, columns, pl.program_id(0))
    hidden = inv_sqrt * jnp.maximum(inv_sqrt * aggregated + bias[...], 0.0)
    result = jnp.dot(w_outer[...], hidden.astype(jnp.bfloat16), preferred_element_type=jnp.float32)
    scores[0] = result.astype(jnp.bfloat16)


def outer_kernel(tile_col, tiles, local, arrived, degrees, bias, logits, columns, sems):
    load_columns(local, arrived, columns, sems)
    inv_sqrt = lax.rsqrt(degrees[...].astype(jnp.float32))
    aggregated = summed(tile_col, tiles, columns, pl.program_id(0))
    result = inv_sqrt * aggregated + bias[...]
    logits[...] = jnp.transpose(result)[:, : logits.shape[1]]


VMEM_LIMIT = 60 * 1024 * 1024


def whole(shape):
    return pl.BlockSpec(shape, lambda step: (0,) * len(shape))


def params():
    return pltpu.CompilerParams(
        dimension_semantics=("arbitrary",), vmem_limit_bytes=VMEM_LIMIT
    )


def on_device(features, w_inner, bias_inner, w_outer, bias_outer, tiles, tile_col, degrees, send_rows):
    send = send_rows[0]
    rows, depth = features.shape
    hidden = w_inner.shape[1]
    classes = w_outer.shape[1]
    padded = 16 * ((classes + 15) // 16)
    peers = send.shape[0]
    blocks, per_block = tile_col.shape
    degrees = degrees.reshape(1, rows)
    parts = rows // CHUNK

    lists, local = pl.pallas_call(
        project_kernel,
        grid=(peers // LISTS,),
        out_shape=(
            jax.ShapeDtypeStruct((peers, hidden, BLOCK), jnp.bfloat16),
            jax.ShapeDtypeStruct((blocks, hidden, BLOCK), jnp.bfloat16),
        ),
        in_specs=[
            whole((rows, depth)),
            whole((depth, hidden)),
            whole((1, rows)),
            pl.BlockSpec((LISTS, BLOCK), lambda step: (step, 0)),
        ],
        out_specs=(
            pl.BlockSpec((LISTS, hidden, BLOCK), lambda step: (step, 0, 0)),
            whole((blocks, hidden, BLOCK)),
        ),
        scratch_shapes=[pltpu.VMEM((parts * hidden, CHUNK), jnp.bfloat16)],
        compiler_params=params(),
    )(features, w_inner, degrees, send)

    def aggregate(body, local, arrived, extras, extra_specs, out_shape, out_spec):
        width = local.shape[1]
        return pl.pallas_call(
            body,
            grid=(blocks,),
            out_shape=out_shape,
            in_specs=[
                pl.BlockSpec(memory_space=pltpu.SMEM),
                pl.BlockSpec((1, per_block, BLOCK, BLOCK), lambda step: (step, 0, 0, 0)),
                pl.BlockSpec(memory_space=pl.ANY),
                pl.BlockSpec(memory_space=pl.ANY),
                pl.BlockSpec((1, BLOCK), lambda step: (0, step)),
            ]
            + extra_specs,
            out_specs=out_spec,
            scratch_shapes=[
                pltpu.VMEM((blocks + peers, width, BLOCK), jnp.bfloat16),
                pltpu.SemaphoreType.DMA((2,)),
            ],
            compiler_params=params(),
        )(tile_col, tiles, local, arrived, degrees, *extras)

    arrived = lax.all_to_all(lists, ("dom", "sub"), split_axis=0, concat_axis=0, tiled=True)
    w_padded = jnp.pad(w_outer.T, ((0, padded - classes), (0, 0)))
    scores = aggregate(
        inner_kernel,
        local,
        arrived,
        (bias_inner.reshape(hidden, 1), w_padded),
        [whole((hidden, 1)), whole((padded, hidden))],
        jax.ShapeDtypeStruct((blocks, padded, BLOCK), jnp.bfloat16),
        pl.BlockSpec((1, padded, BLOCK), lambda step: (step, 0, 0)),
    )

    lists = pl.pallas_call(
        gather_kernel,
        grid=(peers // LISTS,),
        out_shape=jax.ShapeDtypeStruct((peers, padded, BLOCK), jnp.bfloat16),
        in_specs=[
            whole((blocks, padded, BLOCK)),
            pl.BlockSpec((LISTS, BLOCK), lambda step: (step, 0)),
        ],
        out_specs=pl.BlockSpec((LISTS, padded, BLOCK), lambda step: (step, 0, 0)),
        scratch_shapes=[pltpu.VMEM((parts * padded, CHUNK), jnp.bfloat16)],
        compiler_params=params(),
    )(scores, send)

    arrived = lax.all_to_all(lists, ("dom", "sub"), split_axis=0, concat_axis=0, tiled=True)
    bias_padded = jnp.pad(bias_outer, (0, padded - classes)).reshape(padded, 1)
    return aggregate(
        outer_kernel,
        scores,
        arrived,
        (bias_padded,),
        [whole((padded, 1))],
        jax.ShapeDtypeStruct((rows, classes), jnp.float32),
        pl.BlockSpec((BLOCK, classes), lambda step: (step, 0)),
    )


def solution(mesh):
    return jax.shard_map(
        on_device,
        mesh=mesh,
        in_specs=(
            P(("dom", "sub"), None),
            P(),
            P(),
            P(),
            P(),
            P(("dom", "sub"), None, None, None),
            P(("dom", "sub"), None),
            P(("dom", "sub")),
            P(("dom", "sub"), None, None),
        ),
        out_specs=P(("dom", "sub"), None),
        check_vma=False,
    )
```

```python
import functools

import jax
import jax.numpy as jnp
from jax import lax
from jax.experimental import pallas as pl
from jax.experimental.pallas import tpu as pltpu
from jax.sharding import PartitionSpec as P

BLOCK = 128
CHUNK = 256
SIDE = 4
CORES = 2
AXES = 3
CHIPS = SIDE * SIDE
PLANE = CHIPS * CORES
MESH = pl.DeviceIdType.MESH
VMEM_LIMIT = 60 * 1024 * 1024


def pick_rows(stacked, lists, width):
    parts = stacked.shape[0] // width
    index = jnp.concatenate([lists[0:1], lists[1:2]], axis=1)
    low = index & (CHUNK - 1)
    high = lax.shift_right_arithmetic(index, 8)
    lane = lax.broadcasted_iota(jnp.int32, (CHUNK, 2 * BLOCK), 0)
    onehot = jnp.where(lane == low, 1.0, 0.0).astype(jnp.bfloat16)
    found = jnp.dot(stacked, onehot, preferred_element_type=jnp.float32)
    total = jnp.zeros((width, 2 * BLOCK), jnp.float32)
    for part in range(parts):
        total = jnp.where(high == part, found[part * width : (part + 1) * width], total)
    return total.astype(jnp.bfloat16)


class Place:
    def __init__(self):
        dom, sub = lax.axis_index("dom"), lax.axis_index("sub")
        self.at = (dom // SIDE, dom % SIDE, sub // CORES)
        self.core = sub % CORES

    def line(self, f):
        return self.at[f]

    def plane(self, f):
        return [self.at[k] for k in range(AXES) if k != f]

    def device(self, f, a, i, j, core):
        spot = [i, j]
        spot.insert(f, a)
        return (spot[0] * SIDE + spot[1], spot[2] * CORES + core)


def chips(f, a, i, j):
    spot = [i, j]
    spot.insert(f, a)
    return tuple(spot)


class Exchange:
    def __init__(self, place, sizes, held, lists, staged, columns, sems):
        self.place, self.sizes, self.held, self.lists = place, sizes, held, lists
        self.staged, self.columns = staged, columns
        self.line_sent, self.line_got, self.sent, self.got = sems
        self.starts = [sum(sizes[:f]) for f in range(AXES)]

    def along_line(self, f, step):
        p = self.place
        a = p.line(f)
        i, j = p.plane(f)
        return pltpu.make_async_remote_copy(
            src_ref=self.held[f].at[a],
            dst_ref=self.held[f].at[a],
            send_sem=self.line_sent.at[f, step - 1],
            recv_sem=self.line_got.at[f, step - 1],
            device_id=p.device(f, (a + step) % SIDE, i, j, p.core),
            device_id_type=MESH,
        )

    def across(self, f, spot, core):
        p = self.place
        i, j = p.plane(f)
        target = ((i + spot // SIDE) % SIDE, (j + spot % SIDE) % SIDE)
        there = self.columns.at[
            chips(f, pl.ds(0, SIDE), i, j)
            + (p.core, pl.ds(self.starts[f], self.sizes[f]), slice(None))
        ]
        return pltpu.make_async_remote_copy(
            src_ref=self.staged[f].at[spot * CORES + core],
            dst_ref=there,
            send_sem=self.sent.at[f, spot * CORES + core],
            recv_sem=self.got.at[f, spot * CORES + p.core],
            device_id=p.device(f, p.line(f), target[0], target[1], core),
            device_id_type=MESH,
        )

    def arrival(self, f, spot, core):
        p = self.place
        i, j = p.plane(f)
        there = self.columns.at[
            chips(f, pl.ds(0, SIDE), i, j)
            + (p.core, pl.ds(self.starts[f], self.sizes[f]), slice(None))
        ]
        return pltpu.make_async_remote_copy(
            src_ref=self.staged[f].at[spot * CORES],
            dst_ref=there,
            send_sem=self.sent.at[f, spot * CORES],
            recv_sem=self.got.at[f, spot * CORES + core],
            device_id=p.device(f, p.line(f), i, j, 1 - p.core),
            device_id_type=MESH,
        )

    def start_lines(self):
        for f in range(AXES):
            for step in range(1, SIDE):
                self.along_line(f, step).start()

    def wait_lines(self):
        for f in range(AXES):
            for step in range(1, SIDE):
                self.along_line(f, step).wait()

    def run_planes(self):
        p = self.place

        @pl.loop(0, CHIPS)
        def _(turn):
            spot = (turn + 1) % CHIPS
            for f in range(AXES):
                i, j = p.plane(f)
                i, j = (i + spot // SIDE) % SIDE, (j + spot % SIDE) % SIDE
                for a in range(SIDE):
                    picked = pick_rows(self.held[f][a], self.lists[f, a, i, j], self.sizes[f])
                    self.staged[f][spot * CORES, a] = picked[:, :BLOCK]
                    self.staged[f][spot * CORES + 1, a] = picked[:, BLOCK:]
                for core in range(CORES):

                    @pl.when(jnp.logical_or(spot != 0, p.core != core))
                    def _():
                        self.across(f, spot, core).start()

        for f in range(AXES):
            i, j = p.plane(f)
            for a in range(SIDE):
                x, y, z = chips(f, a, i, j)
                rows = pl.ds(self.starts[f], self.sizes[f])
                self.columns[x, y, z, p.core, rows, :] = self.staged[f][p.core, a]

        @pl.loop(0, CHIPS)
        def _(spot):
            for f in range(AXES):
                for core in range(CORES):

                    @pl.when(jnp.logical_or(spot != 0, p.core != core))
                    def _():
                        self.across(f, spot, core).wait_send()
                        self.arrival(f, spot, core).wait_recv()


def summed(tile_col, tiles, columns, row):
    total = None

    def column(t):
        c = (tile_col[row, t] + SIDE * PLANE) % (SIDE * PLANE + 8)
        return columns[c // PLANE, (c // 8) % SIDE, (c // CORES) % SIDE, c % CORES]

    for pair in range(tiles.shape[1] // 2):
        rows = jnp.concatenate([column(2 * pair), column(2 * pair + 1)], axis=1)
        edges = jnp.concatenate([tiles[row, 2 * pair], tiles[row, 2 * pair + 1]], axis=1)
        product = lax.dot_general(
            rows, edges, (((1,), (1,)), ((), ())), preferred_element_type=jnp.float32
        )
        total = product if total is None else total + product
    return total


def kernel(sizes_in, sizes_out, *refs):
    (features, w_inner, bias_inner, w_outer, bias_outer, tiles_far, tile_col, degrees, send) = refs[:9]
    logits = refs[9]
    scratch = list(refs[10:])
    tiles, tiles_sem, lists, list_sent, list_got = scratch[:5]
    held_in, staged_in = scratch[5:8], scratch[8:11]
    held_out, staged_out = scratch[11:14], scratch[14:17]
    columns_in, columns_out = scratch[17:19]
    sems_in, sems_out = scratch[19:23], scratch[23:27]

    place = Place()
    load = pltpu.make_async_copy(tiles_far, tiles, tiles_sem)
    load.start()

    barrier = pltpu.get_barrier_semaphore()

    @pl.loop(0, CHIPS)
    def _(spot):
        for f in range(AXES):
            i, j = place.plane(f)
            i, j = (i + spot // SIDE) % SIDE, (j + spot % SIDE) % SIDE
            for core in range(CORES):

                @pl.when(jnp.logical_or(spot != 0, place.core != core))
                def _():
                    pl.semaphore_signal(
                        barrier,
                        inc=1,
                        device_id=place.device(f, place.line(f), i, j, core),
                        device_id_type=MESH,
                    )

    pl.semaphore_wait(barrier, AXES * (PLANE - 1))

    def lists_along(f, step):
        a = place.line(f)
        there = (a + step) % SIDE
        i, j = place.plane(f)
        cut = [slice(None), slice(None)]
        cut.insert(f, there)
        return pltpu.make_async_remote_copy(
            src_ref=send.at[tuple(cut)],
            dst_ref=lists.at[f, a],
            send_sem=list_sent.at[f, step - 1],
            recv_sem=list_got.at[f, step - 1],
            device_id=place.device(f, there, i, j, place.core),
            device_id_type=MESH,
        )

    for f in range(AXES):
        for step in range(1, SIDE):
            lists_along(f, step).start()

    inner = Exchange(place, sizes_in, held_in, lists, staged_in, columns_in, sems_in)
    outer = Exchange(place, sizes_out, held_out, lists, staged_out, columns_out, sems_out)

    def keep(exchange, part, piece):
        for f in range(AXES):
            size = exchange.sizes[f]
            rows = piece[exchange.starts[f] : exchange.starts[f] + size]
            exchange.held[f][place.line(f), pl.ds(part * size, size), :] = rows
        exchange.columns[SIDE, 0, part, 0] = piece[:, :BLOCK]
        exchange.columns[SIDE, 0, part, 1] = piece[:, BLOCK:]

    def scale(part):
        return lax.rsqrt(degrees[:, pl.ds(part * CHUNK, CHUNK)].astype(jnp.float32))

    for part in range(SIDE):
        product = lax.dot_general(
            w_inner[...],
            features[:, part * CHUNK : (part + 1) * CHUNK],
            (((0,), (0,)), ((), ())),
            preferred_element_type=jnp.float32,
        )
        keep(inner, part, (product * scale(part)).astype(jnp.bfloat16))

    inner.start_lines()
    for f in range(AXES):
        a = place.line(f)
        if f == 0:
            lists[f, a] = send[a]
        elif f == 1:
            lists[f, a] = send[:, a]
        else:
            lists[f, a] = send[:, :, a]
    for f in range(AXES):
        for step in range(1, SIDE):
            lists_along(f, step).wait()
    inner.wait_lines()
    inner.run_planes()

    load.wait()

    @pl.loop(0, SIDE)
    def _(part):
        inv_sqrt = scale(part)
        aggregated = jnp.concatenate(
            [summed(tile_col, tiles, columns_in, 2 * part + half) for half in range(2)], axis=1
        )
        hidden = inv_sqrt * jnp.maximum(inv_sqrt * aggregated + bias_inner[...], 0.0)
        result = jnp.dot(w_outer[...], hidden.astype(jnp.bfloat16), preferred_element_type=jnp.float32)
        keep(outer, part, result.astype(jnp.bfloat16))

    outer.start_lines()
    outer.wait_lines()
    outer.run_planes()

    @pl.loop(0, SIDE)
    def _(part):
        aggregated = jnp.concatenate(
            [summed(tile_col, tiles, columns_out, 2 * part + half) for half in range(2)], axis=1
        )
        result = scale(part) * aggregated + bias_outer[...]
        logits[:, pl.ds(part * CHUNK, CHUNK)] = result[: logits.shape[0]]


def on_device(features, w_inner, bias_inner, w_outer, bias_outer, tiles, tile_col, degrees, send_rows):
    rows, _ = features.shape
    hidden = w_inner.shape[1]
    classes = w_outer.shape[1]
    padded = 16 * AXES
    sizes_in, sizes_out = (96, 80, 80), (16, 16, 16)
    send = send_rows.reshape(SIDE, SIDE, SIDE, CORES, BLOCK)
    vmem = pl.BlockSpec(memory_space=pltpu.VMEM)
    bf16 = jnp.bfloat16

    def held(sizes):
        return [pltpu.VMEM((SIDE, SIDE * size, CHUNK), bf16) for size in sizes]

    def staged(sizes):
        return [pltpu.VMEM((PLANE, SIDE, size, BLOCK), bf16) for size in sizes]

    def columns(sizes):
        return pltpu.VMEM((SIDE + 1, SIDE, SIDE, CORES, sum(sizes), BLOCK), bf16)

    def sems():
        few, many = pltpu.SemaphoreType.DMA((AXES, SIDE - 1)), pltpu.SemaphoreType.DMA((AXES, PLANE))
        return [few, few, many, many]

    return pl.pallas_call(
        functools.partial(kernel, sizes_in, sizes_out),
        out_shape=jax.ShapeDtypeStruct((classes, rows), jnp.float32),
        in_specs=[
            vmem,
            vmem,
            vmem,
            vmem,
            vmem,
            pl.BlockSpec(memory_space=pl.ANY),
            pl.BlockSpec(memory_space=pltpu.SMEM),
            vmem,
            vmem,
        ],
        out_specs=vmem,
        scratch_shapes=[
            pltpu.VMEM(tiles.shape, bf16),
            pltpu.SemaphoreType.DMA,
            pltpu.VMEM((AXES, SIDE, SIDE, SIDE, CORES, BLOCK), jnp.int32),
            pltpu.SemaphoreType.DMA((AXES, SIDE - 1)),
            pltpu.SemaphoreType.DMA((AXES, SIDE - 1)),
            *held(sizes_in),
            *staged(sizes_in),
            *held(sizes_out),
            *staged(sizes_out),
            columns(sizes_in),
            columns(sizes_out),
            *sems(),
            *sems(),
        ],
        compiler_params=pltpu.CompilerParams(
            collective_id=0, has_side_effects=True, vmem_limit_bytes=VMEM_LIMIT
        ),
    )(
        features.T,
        w_inner,
        bias_inner.reshape(hidden, 1),
        jnp.pad(w_outer.T, ((0, padded - classes), (0, 0))),
        jnp.pad(bias_outer, (0, padded - classes)).reshape(padded, 1),
        tiles,
        tile_col,
        degrees.reshape(1, rows),
        send,
    ).T


def solution(mesh):
    return jax.shard_map(
        on_device,
        mesh=mesh,
        in_specs=(
            P(("dom", "sub"), None),
            P(),
            P(),
            P(),
            P(),
            P(("dom", "sub"), None, None, None),
            P(("dom", "sub"), None),
            P(("dom", "sub")),
            P(("dom", "sub"), None, None),
        ),
        out_specs=P(("dom", "sub"), None),
        check_vma=False,
    )
```

```python
import functools

import jax
import jax.numpy as jnp
from jax import lax
from jax.experimental import pallas as pl
from jax.experimental.pallas import tpu as pltpu
from jax.sharding import PartitionSpec as P

BLOCK = 128
CHUNK = 256
SIDE = 4
CORES = 2
AXES = 3
CHIPS = SIDE * SIDE
PLANE = CHIPS * CORES
MESH = pl.DeviceIdType.MESH
VMEM_LIMIT = 60 * 1024 * 1024


def pick_rows(stacked, lists, width):
    parts = stacked.shape[0] // width
    index = jnp.concatenate([lists[0:1], lists[1:2]], axis=1)
    low = index & (CHUNK - 1)
    high = lax.shift_right_arithmetic(index, 8)
    lane = lax.broadcasted_iota(jnp.int32, (CHUNK, 2 * BLOCK), 0)
    onehot = jnp.where(lane == low, 1.0, 0.0).astype(jnp.bfloat16)
    found = jnp.dot(stacked, onehot, preferred_element_type=jnp.float32)
    total = jnp.zeros((width, 2 * BLOCK), jnp.float32)
    for part in range(parts):
        total = jnp.where(high == part, found[part * width : (part + 1) * width], total)
    return total.astype(jnp.bfloat16)


class Place:
    def __init__(self):
        dom, sub = lax.axis_index("dom"), lax.axis_index("sub")
        self.at = (dom // SIDE, dom % SIDE, sub // CORES)
        self.core = sub % CORES

    def turned(self, f):
        return [self.at[(f + k) % AXES] for k in range(AXES)]

    def device(self, f, a, b, c, core):
        x, y, z = natural(f, a, b, c)
        return (x * SIDE + y, z * CORES + core)


def natural(f, a, b, c):
    spot = [None] * AXES
    for k, value in enumerate((a, b, c)):
        spot[(f + k) % AXES] = value
    return tuple(spot)


def remote(source, there, sent, got, device):
    return pltpu.make_async_remote_copy(
        src_ref=source,
        dst_ref=there,
        send_sem=sent,
        recv_sem=got,
        device_id=device,
        device_id_type=MESH,
    )


class Exchange:
    def __init__(self, place, sizes, held, lists, staged, columns, sems):
        self.place, self.sizes, self.held, self.lists = place, sizes, held, lists
        self.staged, self.columns = staged, columns
        self.line, self.near, self.far, self.last = sems
        self.starts = [sum(sizes[:f]) for f in range(AXES)]

    def along_line(self, f, step):
        a, b, c = self.place.turned(f)
        block = self.held[f].at[b, a]
        sems = [self.line.at[k, f, step - 1] for k in range(2)]
        return remote(block, block, *sems, self.place.device(f, (a + step) % SIDE, b, c, self.place.core))

    def to_near(self, f, way, step):
        a, b, c = self.place.turned(f)
        block = self.held[f].at[b, (a + step) % SIDE]
        sems = [self.near.at[k, f, way, step] for k in range(2)]
        there = (b + 1 + 2 * way) % SIDE
        return remote(block, block, *sems, self.place.device(f, a, there, c, self.place.core))

    def to_far(self, f, step):
        a, b, c = self.place.turned(f)
        way = step % 2
        block = self.held[f].at[(b + 3 + 2 * way) % SIDE, (a + step) % SIDE]
        sems = [self.far.at[k, f, step] for k in range(2)]
        there = (b + 1 + 2 * way) % SIDE
        return remote(block, block, *sems, self.place.device(f, a, there, c, self.place.core))

    def to_last(self, f, spot, core, sender, device):
        a, b, c = self.place.turned(f)
        x, y, z = natural(f, pl.ds(0, SIDE), (b + spot // SIDE) % SIDE, c)
        there = self.columns.at[x, y, z, self.place.core, pl.ds(self.starts[f], self.sizes[f]), :]
        return remote(
            self.staged[f].at[spot * CORES + core],
            there,
            self.last.at[0, f, spot * CORES + core],
            self.last.at[1, f, spot * CORES + sender],
            self.place.device(f, a, b, (c + spot % SIDE) % SIDE, device),
        )

    def leaves(self, spot, core):
        return jnp.logical_or(spot % SIDE != 0, self.place.core != core)

    def start(self):
        for step in range(1, SIDE):
            for f in range(AXES):
                self.along_line(f, step).start()
        for way in range(2):
            for f in range(AXES):
                self.to_near(f, way, 0).start()

    def run(self):
        for step in range(1, SIDE):
            for f in range(AXES):
                self.along_line(f, SIDE - step).wait()
            for way in range(2):
                for f in range(AXES):
                    self.to_near(f, way, step).start()
        self.pick(0, SIDE)
        for step in range(SIDE):
            for way in range(2):
                for f in range(AXES):
                    self.to_near(f, way, step).wait()
            for f in range(AXES):
                self.to_far(f, step).start()
        self.pick(SIDE, 2 * SIDE)
        for step in range(SIDE):
            for f in range(AXES):
                self.to_far(f, step).wait()
        self.pick(3 * SIDE, SIDE)
        self.finish()

    def pick(self, first, count):
        p = self.place

        @pl.loop(first, first + count)
        def _(turn):
            row = turn // SIDE
            row = row + jnp.where(row == 2, 1, 0) - jnp.where(row == 3, 1, 0)
            ahead = (turn + 1) % SIDE
            spot = row * SIDE + ahead
            for f in range(AXES):
                a, b, c = p.turned(f)
                b, c = (b + row) % SIDE, (c + ahead) % SIDE
                for k in range(SIDE):
                    picked = pick_rows(self.held[f][b, k], self.lists[f, b, k, c], self.sizes[f])
                    self.staged[f][spot * CORES, k] = picked[:, :BLOCK]
                    self.staged[f][spot * CORES + 1, k] = picked[:, BLOCK:]
                for core in range(CORES):

                    @pl.when(self.leaves(spot, core))
                    def _():
                        self.to_last(f, spot, core, p.core, core).start()

    def finish(self):
        p = self.place
        for f in range(AXES):
            a, b, c = p.turned(f)
            rows = pl.ds(self.starts[f], self.sizes[f])
            for row in range(SIDE):
                for k in range(SIDE):
                    x, y, z = natural(f, k, (b + row) % SIDE, c)
                    self.columns[x, y, z, p.core, rows, :] = self.staged[f][row * PLANE // SIDE + p.core, k]

        @pl.loop(0, CHIPS)
        def _(spot):
            for f in range(AXES):
                for core in range(CORES):

                    @pl.when(self.leaves(spot, core))
                    def _():
                        self.to_last(f, spot, core, p.core, core).wait_send()
                        self.to_last(f, spot, core, core, 1 - p.core).wait_recv()


def summed(tile_col, tiles, columns, row):
    total = None

    def column(t):
        c = (tile_col[row, t] + SIDE * PLANE) % (SIDE * PLANE + 8)
        return columns[c // PLANE, (c // 8) % SIDE, (c // CORES) % SIDE, c % CORES]

    for pair in range(tiles.shape[1] // 2):
        rows = jnp.concatenate([column(2 * pair), column(2 * pair + 1)], axis=1)
        edges = jnp.concatenate([tiles[row, 2 * pair], tiles[row, 2 * pair + 1]], axis=1)
        product = lax.dot_general(
            rows, edges, (((1,), (1,)), ((), ())), preferred_element_type=jnp.float32
        )
        total = product if total is None else total + product
    return total


def kernel(sizes_in, sizes_out, *refs):
    (features, w_inner, bias_inner, w_outer, bias_outer, tiles_far, tile_col, degrees, send) = refs[:9]
    logits = refs[9]
    scratch = list(refs[10:])
    tiles, tiles_sem, lists, list_sems = scratch[:4]
    held_in, staged_in = scratch[4:7], scratch[7:10]
    held_out, staged_out = scratch[10:13], scratch[13:16]
    columns_in, columns_out = scratch[16:18]
    sems_in, sems_out = scratch[18:22], scratch[22:26]

    place = Place()
    load = pltpu.make_async_copy(tiles_far, tiles, tiles_sem)
    load.start()

    barrier = pltpu.get_barrier_semaphore()

    def greet(device):
        pl.semaphore_signal(barrier, inc=1, device_id=device, device_id_type=MESH)

    for f in range(AXES):
        a, b, c = place.turned(f)
        for spot in range(1, CHIPS):
            greet(place.device(f, (a + spot // SIDE) % SIDE, (b + spot % SIDE) % SIDE, c, place.core))
        for step in range(1, SIDE):
            greet(place.device(f, a, b, (c + step) % SIDE, 1 - place.core))
    greet(place.device(0, *place.at, 1 - place.core))

    def lists_to(f, spot):
        a, b, c = place.turned(f)
        there = ((a + spot // SIDE) % SIDE, (b + spot % SIDE) % SIDE)
        return remote(
            send.at[natural(f, *there, slice(None))],
            lists.at[f, b, a],
            list_sems.at[0, f, spot],
            list_sems.at[1, f, spot],
            place.device(f, *there, c, place.core),
        )

    inner = Exchange(place, sizes_in, held_in, lists, staged_in, columns_in, sems_in)
    outer = Exchange(place, sizes_out, held_out, lists, staged_out, columns_out, sems_out)

    def keep(exchange, part, piece):
        for f in range(AXES):
            size = exchange.sizes[f]
            rows = piece[exchange.starts[f] : exchange.starts[f] + size]
            a, b, c = place.turned(f)
            exchange.held[f][b, a, pl.ds(part * size, size), :] = rows
        exchange.columns[SIDE, 0, part, 0] = piece[:, :BLOCK]
        exchange.columns[SIDE, 0, part, 1] = piece[:, BLOCK:]

    def scale(part):
        return lax.rsqrt(degrees[:, pl.ds(part * CHUNK, CHUNK)].astype(jnp.float32))

    for part in range(SIDE):
        product = lax.dot_general(
            w_inner[...],
            features[:, part * CHUNK : (part + 1) * CHUNK],
            (((0,), (0,)), ((), ())),
            preferred_element_type=jnp.float32,
        )
        keep(inner, part, (product * scale(part)).astype(jnp.bfloat16))

    for f in range(AXES):
        a, b, c = place.turned(f)
        x, y, z = natural(f, a, b, slice(None))
        lists[f, b, a] = send[x, y, z]

    pl.semaphore_wait(barrier, AXES * (CHIPS - 1 + SIDE - 1) + 1)
    for f in range(AXES):
        for spot in range(1, CHIPS):
            lists_to(f, spot).start()
    inner.start()
    for f in range(AXES):
        for spot in range(1, CHIPS):
            lists_to(f, spot).wait()
    inner.run()

    load.wait()

    @pl.loop(0, SIDE)
    def _(part):
        inv_sqrt = scale(part)
        aggregated = jnp.concatenate(
            [summed(tile_col, tiles, columns_in, 2 * part + half) for half in range(2)], axis=1
        )
        hidden = inv_sqrt * jnp.maximum(inv_sqrt * aggregated + bias_inner[...], 0.0)
        result = jnp.dot(w_outer[...], hidden.astype(jnp.bfloat16), preferred_element_type=jnp.float32)
        keep(outer, part, result.astype(jnp.bfloat16))

    outer.start()
    outer.run()

    @pl.loop(0, SIDE)
    def _(part):
        aggregated = jnp.concatenate(
            [summed(tile_col, tiles, columns_out, 2 * part + half) for half in range(2)], axis=1
        )
        result = scale(part) * aggregated + bias_outer[...]
        logits[:, pl.ds(part * CHUNK, CHUNK)] = result[: logits.shape[0]]


def on_device(features, w_inner, bias_inner, w_outer, bias_outer, tiles, tile_col, degrees, send_rows):
    rows, _ = features.shape
    hidden = w_inner.shape[1]
    classes = w_outer.shape[1]
    padded = 16 * AXES
    sizes_in, sizes_out = (96, 80, 80), (16, 16, 16)
    send = send_rows.reshape(SIDE, SIDE, SIDE, CORES, BLOCK)
    vmem = pl.BlockSpec(memory_space=pltpu.VMEM)
    bf16 = jnp.bfloat16

    def held(sizes):
        return [pltpu.VMEM((SIDE, SIDE, SIDE * size, CHUNK), bf16) for size in sizes]

    def staged(sizes):
        return [pltpu.VMEM((PLANE, SIDE, size, BLOCK), bf16) for size in sizes]

    def columns(sizes):
        return pltpu.VMEM((SIDE + 1, SIDE, SIDE, CORES, sum(sizes), BLOCK), bf16)

    def sems():
        shapes = [(SIDE - 1,), (2, SIDE), (SIDE,), (PLANE,)]
        return [pltpu.SemaphoreType.DMA((2, AXES, *shape)) for shape in shapes]

    return pl.pallas_call(
        functools.partial(kernel, sizes_in, sizes_out),
        out_shape=jax.ShapeDtypeStruct((classes, rows), jnp.float32),
        in_specs=[
            vmem,
            vmem,
            vmem,
            vmem,
            vmem,
            pl.BlockSpec(memory_space=pl.ANY),
            pl.BlockSpec(memory_space=pltpu.SMEM),
            vmem,
            vmem,
        ],
        out_specs=vmem,
        scratch_shapes=[
            pltpu.VMEM(tiles.shape, bf16),
            pltpu.SemaphoreType.DMA,
            pltpu.VMEM((AXES, SIDE, SIDE, SIDE, CORES, BLOCK), jnp.int32),
            pltpu.SemaphoreType.DMA((2, AXES, CHIPS)),
            *held(sizes_in),
            *staged(sizes_in),
            *held(sizes_out),
            *staged(sizes_out),
            columns(sizes_in),
            columns(sizes_out),
            *sems(),
            *sems(),
        ],
        compiler_params=pltpu.CompilerParams(
            collective_id=0, has_side_effects=True, vmem_limit_bytes=VMEM_LIMIT
        ),
    )(
        features.T,
        w_inner,
        bias_inner.reshape(hidden, 1),
        jnp.pad(w_outer.T, ((0, padded - classes), (0, 0))),
        jnp.pad(bias_outer, (0, padded - classes)).reshape(padded, 1),
        tiles,
        tile_col,
        degrees.reshape(1, rows),
        send,
    ).T


def solution(mesh):
    return jax.shard_map(
        on_device,
        mesh=mesh,
        in_specs=(
            P(("dom", "sub"), None),
            P(),
            P(),
            P(),
            P(),
            P(("dom", "sub"), None, None, None),
            P(("dom", "sub"), None),
            P(("dom", "sub")),
            P(("dom", "sub"), None, None),
        ),
        out_specs=P(("dom", "sub"), None),
        check_vma=False,
    )
```

```python
import functools

import jax
import jax.numpy as jnp
from jax import lax
from jax.experimental import pallas as pl
from jax.experimental.pallas import tpu as pltpu
from jax.sharding import PartitionSpec as P

BLOCK = 128
CHUNK = 256
SIDE = 4
CORES = 2
AXES = 3
CHIPS = SIDE * SIDE
PLANE = CHIPS * CORES
MESH = pl.DeviceIdType.MESH
VMEM_LIMIT = 60 * 1024 * 1024


def pick_rows(stacked, lists, width):
    parts, chunk = stacked.shape[0] // width, stacked.shape[1]
    index = jnp.concatenate([lists[0:1], lists[1:2]], axis=1)
    low = index & (chunk - 1)
    high = lax.shift_right_arithmetic(index, chunk.bit_length() - 1)
    lane = lax.broadcasted_iota(jnp.int32, (chunk, 2 * BLOCK), 0)
    onehot = jnp.where(lane == low, 1.0, 0.0).astype(jnp.bfloat16)
    found = jnp.dot(stacked, onehot, preferred_element_type=jnp.float32)
    total = jnp.zeros((width, 2 * BLOCK), jnp.float32)
    for part in range(parts):
        total = jnp.where(high == part, found[part * width : (part + 1) * width], total)
    return total.astype(jnp.bfloat16)


class Place:
    def __init__(self):
        dom, sub = lax.axis_index("dom"), lax.axis_index("sub")
        self.at = (dom // SIDE, dom % SIDE, sub // CORES)
        self.core = sub % CORES

    def turned(self, f):
        return [self.at[(f + k) % AXES] for k in range(AXES)]

    def device(self, f, a, b, c, core):
        x, y, z = natural(f, a, b, c)
        return (x * SIDE + y, z * CORES + core)


def natural(f, a, b, c):
    spot = [None] * AXES
    for k, value in enumerate((a, b, c)):
        spot[(f + k) % AXES] = value
    return tuple(spot)


def remote(source, there, sent, got, device):
    return pltpu.make_async_remote_copy(
        src_ref=source,
        dst_ref=there,
        send_sem=sent,
        recv_sem=got,
        device_id=device,
        device_id_type=MESH,
    )


class Exchange:
    def __init__(self, place, sizes, held, lists, staged, columns, sems):
        self.place, self.sizes, self.held, self.lists = place, sizes, held, lists
        self.staged, self.columns = staged, columns
        self.held_sent, self.last_sent, self.line, self.near, self.far, self.last = sems
        self.starts = [sum(sizes[:f]) for f in range(AXES)]

    def along_line(self, f, step):
        a, b, c = self.place.turned(f)
        block = self.held[f].at[b * SIDE + a]
        sems = self.held_sent.at[f], self.line.at[f, step - 1]
        return remote(block, block, *sems, self.place.device(f, (a + step) % SIDE, b, c, self.place.core))

    def to_near(self, f, way, step):
        a, b, c = self.place.turned(f)
        block = self.held[f].at[b * SIDE + (a + step) % SIDE]
        sems = self.held_sent.at[f], self.near.at[f, way, step]
        there = (b + 1 + 2 * way) % SIDE
        return remote(block, block, *sems, self.place.device(f, a, there, c, self.place.core))

    def to_far(self, f, step):
        a, b, c = self.place.turned(f)
        way = step % 2
        block = self.held[f].at[(b + 3 + 2 * way) % SIDE * SIDE + (a + step) % SIDE]
        sems = self.held_sent.at[f], self.far.at[f, step]
        there = (b + 1 + 2 * way) % SIDE
        return remote(block, block, *sems, self.place.device(f, a, there, c, self.place.core))

    def to_last(self, f, spot, core):
        a, b, c = self.place.turned(f)
        x, y, z = natural(f, pl.ds(0, SIDE), (b + spot // SIDE) % SIDE, c)
        there = self.columns.at[x, y, z, self.place.core, pl.ds(self.starts[f], self.sizes[f]), :]
        return remote(
            self.staged[f].at[spot * CORES + core],
            there,
            self.last_sent.at[f],
            self.last.at[f],
            self.place.device(f, a, b, (c + spot % SIDE) % SIDE, core),
        )

    def leaves(self, spot, core):
        return jnp.logical_or(spot % SIDE != 0, self.place.core != core)

    def start(self):
        for step in range(1, SIDE):
            for f in range(AXES):
                self.along_line(f, step).start()
        for way in range(2):
            for f in range(AXES):
                self.to_near(f, way, 0).start()

    def run(self, ready=lambda: None):
        for step in range(1, SIDE):
            for f in range(AXES):
                self.along_line(f, SIDE - step).wait_recv()
            for way in range(2):
                for f in range(AXES):
                    self.to_near(f, way, step).start()
        ready()
        self.pick(0, SIDE)
        for step in range(SIDE):
            for way in range(2):
                for f in range(AXES):
                    self.to_near(f, way, step).wait_recv()
            for f in range(AXES):
                self.to_far(f, step).start()
        self.pick(SIDE, 2 * SIDE)
        for step in range(SIDE):
            for f in range(AXES):
                self.to_far(f, step).wait_recv()
        self.pick(3 * SIDE, SIDE)
        self.finish()

    def pick(self, first, count):
        p = self.place

        @pl.loop(first, first + count)
        def _(turn):
            row = turn // SIDE
            row = row + jnp.where(row == 2, 1, 0) - jnp.where(row == 3, 1, 0)
            ahead = (turn + 1) % SIDE
            spot = row * SIDE + ahead
            for f in range(AXES):
                a, b, c = p.turned(f)
                b, c = (b + row) % SIDE, (c + ahead) % SIDE
                for k in range(SIDE):
                    picked = pick_rows(self.held[f][b * SIDE + k], self.lists[f, b, k, c], self.sizes[f])
                    self.staged[f][spot * CORES, k] = picked[:, :BLOCK]
                    self.staged[f][spot * CORES + 1, k] = picked[:, BLOCK:]
                for core in range(CORES):

                    @pl.when(self.leaves(spot, core))
                    def _():
                        self.to_last(f, spot, core).start()

    def finish(self):
        p = self.place
        for f in range(AXES):
            a, b, c = p.turned(f)
            rows = pl.ds(self.starts[f], self.sizes[f])
            for row in range(SIDE):
                for k in range(SIDE):
                    x, y, z = natural(f, k, (b + row) % SIDE, c)
                    self.columns[x, y, z, p.core, rows, :] = self.staged[f][row * PLANE // SIDE + p.core, k]

        for f in range(AXES):
            a, b, c = p.turned(f)
            device = p.device(f, a, b, c, 1 - p.core)
            held = self.held[f].at[pl.ds(0, CHIPS - 1)]
            picked = self.staged[f].at[pl.ds(0, PLANE - SIDE)]
            remote(held, held, self.held_sent.at[f], self.last.at[f], device).wait_send()
            last = remote(picked, picked, self.last_sent.at[f], self.last.at[f], device)
            last.wait_send()
            last.wait_recv()


def summed(tile_col, tiles, columns, row, swap):
    total = None

    def column(t):
        c = (tile_col[row, t] + SIDE * PLANE) % (SIDE * PLANE + 8)
        return columns[c // PLANE, (c // 8) % SIDE, (c // CORES) % SIDE, c % CORES]

    for pair in range(tiles.shape[1] // 2):
        rows = jnp.concatenate([column(2 * pair), column(2 * pair + 1)], axis=1)
        edges = jnp.concatenate([tiles[row, 2 * pair], tiles[row, 2 * pair + 1]], axis=1)
        operands = (edges, rows) if swap else (rows, edges)
        product = lax.dot_general(
            *operands, (((1,), (1,)), ((), ())), preferred_element_type=jnp.float32
        )
        total = product if total is None else total + product
    return total


def down(row):
    return jnp.transpose(jnp.broadcast_to(row, (BLOCK, row.shape[1])))


def kernel(sizes_in, sizes_out, *refs):
    (features_far, w_far, bias_inner, w_outer, bias_outer, tiles_far, tile_col, degrees, send) = refs[:9]
    logits = refs[9]
    scratch = list(refs[10:])
    tiles, tiles_sem, lists, halfway = scratch[:4]
    held_in, staged_in = scratch[4:7], scratch[7:10]
    held_out, staged_out = scratch[10:13], scratch[13:16]
    columns_in, columns_out = scratch[16:18]
    features, w_inner, few_sems, list_sent, list_got, held_sent, last_sent = scratch[18:25]
    sems_in = held_sent, last_sent, *scratch[25:29]
    sems_out = held_sent, last_sent, *scratch[29:33]

    place = Place()
    load_w = pltpu.make_async_copy(w_far, w_inner, few_sems.at[0])
    load_features = pltpu.make_async_copy(features_far, features, few_sems.at[1])
    load = pltpu.make_async_copy(tiles_far, tiles, tiles_sem)
    load_w.start()
    load_features.start()
    load.start()

    barrier = pltpu.get_barrier_semaphore()

    def greet(device):
        pl.semaphore_signal(barrier, inc=1, device_id=device, device_id_type=MESH)

    for f in range(AXES):
        a, b, c = place.turned(f)
        for step in range(1, SIDE):
            for core in range(CORES):
                greet(place.device(f, (a + step) % SIDE, b, c, core))
    greet(place.device(0, *place.at, 1 - place.core))

    def lists_along(f, step):
        a, b, c = place.turned(f)
        there = (a + step) % SIDE
        cut = [slice(None)] * AXES
        cut[f] = there
        return remote(
            send.at[tuple(cut)],
            halfway.at[f, a],
            list_sent.at[0, f],
            list_got.at[0, f],
            place.device(f, there, b, c, place.core),
        )

    def cut_lists(f, b):
        return (f, slice(None), slice(None), b) if f == 1 else (f, slice(None), b)

    def lists_across(f, step):
        a, b, c = place.turned(f)
        there = (b + step) % SIDE
        return remote(
            halfway.at[cut_lists(f, there)],
            lists.at[f, b],
            list_sent.at[1, f],
            list_got.at[1, f],
            place.device(f, a, there, c, place.core),
        )

    def lists_done(f, stage, buffer):
        three = buffer.at[f, pl.ds(0, SIDE - 1)]
        device = place.device(0, *place.at, 1 - place.core)
        return remote(three, three, list_sent.at[stage, f], list_got.at[stage, f], device)

    for f in range(AXES):
        a, b, c = place.turned(f)
        cut = [slice(None)] * AXES
        cut[f] = a
        halfway[f, a] = send[tuple(cut)]

    pl.semaphore_wait(barrier, AXES * (SIDE - 1) * CORES + 1)
    for f in range(AXES):
        for step in range(1, SIDE):
            lists_along(f, step).start()

    def lists_middle():
        for f in range(AXES):
            lists_done(f, 0, halfway).wait_recv()
            for step in range(1, SIDE):
                lists_across(f, step).start()
            a, b, c = place.turned(f)
            lists[f, b] = halfway[cut_lists(f, b)]

    def lists_ready():
        for f in range(AXES):
            lists_done(f, 0, halfway).wait_send()
            lists_done(f, 1, lists).wait()

    inner = Exchange(place, sizes_in, held_in, lists, staged_in, columns_in, sems_in)
    outer = Exchange(place, sizes_out, held_out, lists, staged_out, columns_out, sems_out)

    def keep(exchange, part, piece):
        chunk = exchange.held[0].shape[2]
        for f in range(AXES):
            size = exchange.sizes[f]
            rows = piece[exchange.starts[f] : exchange.starts[f] + size]
            a, b, c = place.turned(f)
            for k in range(CHUNK // chunk):
                at = pl.ds((part * (CHUNK // chunk) + k) * size, size)
                exchange.held[f][b * SIDE + a, at, :] = rows[:, k * chunk : (k + 1) * chunk]
        exchange.columns[SIDE, 0, part, 0] = piece[:, :BLOCK]
        exchange.columns[SIDE, 0, part, 1] = piece[:, BLOCK:]

    def scale(start, size):
        return lax.rsqrt(degrees[:, pl.ds(start, size)].astype(jnp.float32))

    load_w.wait()
    w_turned = jnp.transpose(w_inner[...])
    load_features.wait()
    for part in range(SIDE):
        product = jnp.dot(
            w_turned,
            features[:, part * CHUNK : (part + 1) * CHUNK],
            preferred_element_type=jnp.float32,
        )
        keep(inner, part, (product * scale(part * CHUNK, CHUNK)).astype(jnp.bfloat16))

    inner.start()
    lists_middle()
    inner.run(lists_ready)

    load.wait()
    bias_down = down(bias_inner[...])

    @pl.loop(0, SIDE)
    def _(part):
        hidden = []
        for half in range(2):
            inv_sqrt = scale((2 * part + half) * BLOCK, BLOCK)
            aggregated = summed(tile_col, tiles, columns_in, 2 * part + half, False)
            hidden.append(inv_sqrt * jnp.maximum(inv_sqrt * aggregated + bias_down, 0.0))
        hidden = jnp.concatenate(hidden, axis=1).astype(jnp.bfloat16)
        result = jnp.dot(w_outer[...], hidden, preferred_element_type=jnp.float32)
        spare = jnp.zeros((sum(sizes_out) - result.shape[0], CHUNK), jnp.float32)
        keep(outer, part, jnp.concatenate([result, spare], axis=0).astype(jnp.bfloat16))

    outer.start()
    outer.run()
    last_down = down(bias_outer[...])

    @pl.loop(0, SIDE)
    def _(part):
        for half in range(2):
            start = (2 * part + half) * BLOCK
            aggregated = jnp.transpose(summed(tile_col, tiles, columns_out, 2 * part + half, True))
            logits[:, pl.ds(start, BLOCK)] = scale(start, BLOCK) * aggregated[: logits.shape[0]] + last_down


def on_device(features, w_inner, bias_inner, w_outer, bias_outer, tiles, tile_col, degrees, send_rows):
    rows, _ = features.shape
    hidden = w_inner.shape[1]
    classes = w_outer.shape[1]
    sizes_in, sizes_out = (96, 80, 80), (16, 16, 16)
    send = send_rows.reshape(SIDE, SIDE, SIDE, CORES, BLOCK)
    vmem = pl.BlockSpec(memory_space=pltpu.VMEM)
    bf16 = jnp.bfloat16

    def held(sizes, chunk):
        return [pltpu.VMEM((CHIPS, rows // chunk * size, chunk), bf16) for size in sizes]

    def staged(sizes):
        return [pltpu.VMEM((PLANE, SIDE, size, BLOCK), bf16) for size in sizes]

    def columns(sizes):
        return pltpu.VMEM((SIDE + 1, SIDE, SIDE, CORES, sum(sizes), BLOCK), bf16)

    def sems():
        shapes = [(SIDE - 1,), (2, SIDE), (SIDE,), ()]
        return [pltpu.SemaphoreType.DMA((AXES, *shape)) for shape in shapes]

    return pl.pallas_call(
        functools.partial(kernel, sizes_in, sizes_out),
        out_shape=jax.ShapeDtypeStruct((classes, rows), jnp.float32),
        in_specs=[
            pl.BlockSpec(memory_space=pl.ANY),
            pl.BlockSpec(memory_space=pl.ANY),
            vmem,
            vmem,
            vmem,
            pl.BlockSpec(memory_space=pl.ANY),
            pl.BlockSpec(memory_space=pltpu.SMEM),
            vmem,
            vmem,
        ],
        out_specs=vmem,
        scratch_shapes=[
            pltpu.VMEM(tiles.shape, bf16),
            pltpu.SemaphoreType.DMA,
            pltpu.VMEM((AXES, SIDE, SIDE, SIDE, CORES, BLOCK), jnp.int32),
            pltpu.VMEM((AXES, SIDE, SIDE, SIDE, CORES, BLOCK), jnp.int32),
            *held(sizes_in, CHUNK),
            *staged(sizes_in),
            *held(sizes_out, BLOCK),
            *staged(sizes_out),
            columns(sizes_in),
            columns(sizes_out),
            pltpu.VMEM((features.shape[1], rows), bf16),
            pltpu.VMEM(w_inner.shape, bf16),
            pltpu.SemaphoreType.DMA((2,)),
            pltpu.SemaphoreType.DMA((2, AXES)),
            pltpu.SemaphoreType.DMA((2, AXES)),
            pltpu.SemaphoreType.DMA((AXES,)),
            pltpu.SemaphoreType.DMA((AXES,)),
            *sems(),
            *sems(),
        ],
        compiler_params=pltpu.CompilerParams(
            collective_id=0, has_side_effects=True, vmem_limit_bytes=VMEM_LIMIT
        ),
    )(
        features.T,
        w_inner,
        bias_inner.reshape(1, hidden),
        w_outer.T,
        bias_outer.reshape(1, classes),
        tiles,
        tile_col,
        degrees.reshape(1, rows),
        send,
    ).T


def solution(mesh):
    return jax.shard_map(
        on_device,
        mesh=mesh,
        in_specs=(
            P(("dom", "sub"), None),
            P(),
            P(),
            P(),
            P(),
            P(("dom", "sub"), None, None, None),
            P(("dom", "sub"), None),
            P(("dom", "sub")),
            P(("dom", "sub"), None, None),
        ),
        out_specs=P(("dom", "sub"), None),
        check_vma=False,
    )
```

```python
import functools

import jax
import jax.numpy as jnp
from jax import lax
from jax.experimental import pallas as pl
from jax.experimental.pallas import tpu as pltpu
from jax.sharding import PartitionSpec as P

BLOCK = 128
CHUNK = 256
SIDE = 4
CORES = 2
AXES = 3
CHIPS = SIDE * SIDE
PLANE = CHIPS * CORES
MESH = pl.DeviceIdType.MESH
VMEM_LIMIT = 63 * 1024 * 1024


def pick_rows(stacked, lists, width, kept):
    parts, chunk = stacked.shape[0] // width, stacked.shape[1]
    index = jnp.concatenate([lists[0:1], lists[1:2]], axis=1)
    high = lax.shift_right_arithmetic(index, chunk.bit_length() - 1)
    if chunk == BLOCK:
        onehot = kept[...]
    else:
        low = index & (chunk - 1)
        lane = lax.broadcasted_iota(jnp.int32, (chunk, 2 * BLOCK), 0)
        onehot = jnp.where(lane == low, 1.0, 0.0).astype(jnp.bfloat16)
        kept[...] = onehot[:BLOCK] + onehot[BLOCK:]
    found = jnp.dot(stacked, onehot, preferred_element_type=jnp.float32)
    total = jnp.zeros((width, 2 * BLOCK), jnp.float32)
    for part in range(parts):
        total = jnp.where(high == part, found[part * width : (part + 1) * width], total)
    return total.astype(jnp.bfloat16)


def mod(value, by=SIDE):
    return lax.rem(value, jnp.int32(by))


def div(value, by=SIDE):
    return lax.div(value, jnp.int32(by))


class Place:
    def __init__(self):
        dom, sub = lax.axis_index("dom"), lax.axis_index("sub")
        self.at = (div(dom), mod(dom), div(sub, CORES))
        self.core = mod(sub, CORES)

    def turned(self, f):
        return [self.at[(f + k) % AXES] for k in range(AXES)]

    def device(self, f, a, b, c, core):
        x, y, z = natural(f, a, b, c)
        return (x * SIDE + y, z * CORES + core)


def natural(f, a, b, c):
    spot = [None] * AXES
    for k, value in enumerate((a, b, c)):
        spot[(f + k) % AXES] = value
    return tuple(spot)


def remote(source, there, sent, got, device):
    return pltpu.make_async_remote_copy(
        src_ref=source,
        dst_ref=there,
        send_sem=sent,
        recv_sem=got,
        device_id=device,
        device_id_type=MESH,
    )


class Exchange:
    def __init__(self, place, sizes, held, lists, kept, staged, columns, sems):
        self.kept = kept
        self.place, self.sizes, self.held, self.lists = place, sizes, held, lists
        self.staged, self.columns = staged, columns
        self.held_sent, self.last_sent, self.line, self.near, self.far, self.last = sems
        self.starts = [sum(sizes[:f]) for f in range(AXES)]

    def along_line(self, f, step):
        a, b, c = self.place.turned(f)
        block = self.held[f].at[b * SIDE + a]
        sems = self.held_sent.at[f], self.line.at[f, step - 1]
        return remote(block, block, *sems, self.place.device(f, mod(a + step), b, c, self.place.core))

    def to_near(self, f, way, step):
        a, b, c = self.place.turned(f)
        block = self.held[f].at[b * SIDE + mod(a + step)]
        sems = self.held_sent.at[f], self.near.at[f, way, step]
        there = mod(b + 1 + 2 * way)
        return remote(block, block, *sems, self.place.device(f, a, there, c, self.place.core))

    def to_far(self, f, step):
        a, b, c = self.place.turned(f)
        way = step % 2
        block = self.held[f].at[mod(b + 3 + 2 * way) * SIDE + mod(a + step)]
        sems = self.held_sent.at[f], self.far.at[f, step]
        there = mod(b + 1 + 2 * way)
        return remote(block, block, *sems, self.place.device(f, a, there, c, self.place.core))

    def to_last(self, f, row, ahead, core):
        a, b, c = self.place.turned(f)
        x, y, z = natural(f, pl.ds(0, SIDE), mod(b + row), c)
        there = self.columns.at[x, y, z, self.place.core, pl.ds(self.starts[f], self.sizes[f]), :]
        return remote(
            self.staged[f].at[(row * SIDE + ahead) * CORES + core],
            there,
            self.last_sent.at[f],
            self.last.at[f],
            self.place.device(f, a, b, mod(c + ahead), core),
        )

    def leaves(self, ahead, core):
        return jnp.logical_or(ahead != 0, self.place.core != core)

    def start(self):
        for step in range(1, SIDE):
            for f in range(AXES):
                self.along_line(f, step).start()
        for way in range(2):
            for f in range(AXES):
                self.to_near(f, way, 0).start()

    def run(self, ready=lambda: None):
        for step in range(1, SIDE):
            for f in range(AXES):
                self.along_line(f, SIDE - step).wait_recv()
            for way in range(2):
                for f in range(AXES):
                    self.to_near(f, way, step).start()
        ready()
        self.pick(0, SIDE)
        for step in range(SIDE):
            for way in range(2):
                for f in range(AXES):
                    self.to_near(f, way, step).wait_recv()
            for f in range(AXES):
                self.to_far(f, step).start()
        self.pick(SIDE, 2 * SIDE)
        for step in range(SIDE):
            for f in range(AXES):
                self.to_far(f, step).wait_recv()
        self.pick(3 * SIDE, SIDE)
        self.finish()

    def pick(self, first, count):
        p = self.place

        @pl.loop(first, first + count)
        def _(turn):
            row = div(turn)
            row = row + jnp.where(row == 2, 1, 0) - jnp.where(row == 3, 1, 0)
            ahead = mod(turn + 1)
            spot = row * SIDE + ahead
            for f in range(AXES):
                a, b, c = p.turned(f)
                b, c = mod(b + row), mod(c + ahead)
                for k in range(SIDE):
                    picked = pick_rows(
                        self.held[f][b * SIDE + k],
                        self.lists[f, b, k, c],
                        self.sizes[f],
                        self.kept.at[turn, f, k],
                    )
                    self.staged[f][spot * CORES, k] = picked[:, :BLOCK]
                    self.staged[f][spot * CORES + 1, k] = picked[:, BLOCK:]
            for core in range(CORES):

                @pl.when(self.leaves(ahead, core))
                def _():
                    for f in range(AXES):
                        self.to_last(f, row, ahead, core).start()

    def finish(self):
        p = self.place
        for f in range(AXES):
            a, b, c = p.turned(f)
            rows = pl.ds(self.starts[f], self.sizes[f])
            for row in range(SIDE):
                for k in range(SIDE):
                    x, y, z = natural(f, k, mod(b + row), c)
                    self.columns[x, y, z, p.core, rows, :] = self.staged[f][row * PLANE // SIDE + p.core, k]

        for f in range(AXES):
            a, b, c = p.turned(f)
            device = p.device(f, a, b, c, 1 - p.core)
            held = self.held[f].at[pl.ds(0, CHIPS - 1)]
            picked = self.staged[f].at[pl.ds(0, PLANE - SIDE)]
            remote(held, held, self.held_sent.at[f], self.last.at[f], device).wait_send()
            last = remote(picked, picked, self.last_sent.at[f], self.last.at[f], device)
            last.wait_send()
            last.wait_recv()


def summed(tile_col, tiles, columns, row, swap):
    total = None

    blocks = SIDE * PLANE
    flat = columns.reshape(columns.shape[0] * PLANE, *columns.shape[4:])

    def column(t):
        c = tile_col[row, t]
        return flat[jnp.where(c < 8, c + blocks, c - 8)]

    for pair in range(tiles.shape[1] // 2):
        rows = jnp.concatenate([column(2 * pair), column(2 * pair + 1)], axis=1)
        edges = jnp.concatenate([tiles[row, 2 * pair], tiles[row, 2 * pair + 1]], axis=1)
        operands = (edges, rows) if swap else (rows, edges)
        product = lax.dot_general(
            *operands, (((1,), (1,)), ((), ())), preferred_element_type=jnp.float32
        )
        total = product if total is None else total + product
    return total


def down(row):
    return jnp.transpose(jnp.broadcast_to(row, (BLOCK, row.shape[1])))


def kernel(sizes_in, sizes_out, *refs):
    (features_far, w_far, bias_inner, w_outer, bias_outer, tiles_far, tile_col, degrees, send) = refs[:9]
    logits = refs[9]
    scratch = list(refs[10:])
    tiles, tiles_sem, lists, halfway = scratch[:4]
    held_in, staged_in = scratch[4:7], scratch[7:10]
    held_out, staged_out = scratch[10:13], scratch[13:16]
    columns_in, columns_out = scratch[16:18]
    features, w_inner, few_sems, list_sent, list_got, held_sent, last_sent = scratch[18:25]
    sems_in = held_sent, last_sent, *scratch[25:29]
    sems_out = held_sent, last_sent, *scratch[29:33]
    kept = scratch[33]

    place = Place()
    load_w = pltpu.make_async_copy(w_far, w_inner, few_sems.at[0])
    load_features = pltpu.make_async_copy(features_far, features, few_sems.at[1])
    load = pltpu.make_async_copy(tiles_far, tiles, tiles_sem)
    load_w.start()
    load_features.start()
    load.start()

    barrier = pltpu.get_barrier_semaphore()

    def greet(device):
        pl.semaphore_signal(barrier, inc=1, device_id=device, device_id_type=MESH)

    for f in range(AXES):
        a, b, c = place.turned(f)
        for step in range(1, SIDE):
            for core in range(CORES):
                greet(place.device(f, mod(a + step), b, c, core))
    greet(place.device(0, *place.at, 1 - place.core))

    def lists_along(f, step):
        a, b, c = place.turned(f)
        there = mod(a + step)
        cut = [slice(None)] * AXES
        cut[f] = there
        return remote(
            send.at[tuple(cut)],
            halfway.at[f, a],
            list_sent.at[0, f],
            list_got.at[0, f],
            place.device(f, there, b, c, place.core),
        )

    def cut_lists(f, b):
        return (f, slice(None), slice(None), b) if f == 1 else (f, slice(None), b)

    def lists_across(f, step):
        a, b, c = place.turned(f)
        there = mod(b + step)
        return remote(
            halfway.at[cut_lists(f, there)],
            lists.at[f, b],
            list_sent.at[1, f],
            list_got.at[1, f],
            place.device(f, a, there, c, place.core),
        )

    def lists_done(f, stage, buffer):
        three = buffer.at[f, pl.ds(0, SIDE - 1)]
        device = place.device(0, *place.at, 1 - place.core)
        return remote(three, three, list_sent.at[stage, f], list_got.at[stage, f], device)

    for f in range(AXES):
        a, b, c = place.turned(f)
        cut = [slice(None)] * AXES
        cut[f] = a
        halfway[f, a] = send[tuple(cut)]

    pl.semaphore_wait(barrier, AXES * (SIDE - 1) * CORES + 1)
    for f in range(AXES):
        for step in range(1, SIDE):
            lists_along(f, step).start()

    def lists_middle():
        for f in range(AXES):
            lists_done(f, 0, halfway).wait_recv()
            for step in range(1, SIDE):
                lists_across(f, step).start()
            a, b, c = place.turned(f)
            lists[f, b] = halfway[cut_lists(f, b)]

    def lists_ready():
        for f in range(AXES):
            lists_done(f, 0, halfway).wait_send()
            lists_done(f, 1, lists).wait()

    inner = Exchange(place, sizes_in, held_in, lists, kept, staged_in, columns_in, sems_in)
    outer = Exchange(place, sizes_out, held_out, lists, kept, staged_out, columns_out, sems_out)

    def keep(exchange, part, piece):
        chunk = exchange.held[0].shape[2]
        for f in range(AXES):
            size = exchange.sizes[f]
            rows = piece[exchange.starts[f] : exchange.starts[f] + size]
            a, b, c = place.turned(f)
            for k in range(CHUNK // chunk):
                at = pl.ds((part * (CHUNK // chunk) + k) * size, size)
                exchange.held[f][b * SIDE + a, at, :] = rows[:, k * chunk : (k + 1) * chunk]
        exchange.columns[SIDE, 0, part, 0] = piece[:, :BLOCK]
        exchange.columns[SIDE, 0, part, 1] = piece[:, BLOCK:]

    def scale(start, size):
        return lax.rsqrt(degrees[:, pl.ds(start, size)].astype(jnp.float32))

    load_w.wait()
    w_turned = jnp.transpose(w_inner[...])
    load_features.wait()
    for part in range(SIDE):
        product = jnp.dot(
            w_turned,
            features[:, part * CHUNK : (part + 1) * CHUNK],
            preferred_element_type=jnp.float32,
        )
        keep(inner, part, (product * scale(part * CHUNK, CHUNK)).astype(jnp.bfloat16))

    inner.start()
    lists_middle()
    inner.run(lists_ready)

    load.wait()
    bias_down = down(bias_inner[...])

    @pl.loop(0, SIDE)
    def _(part):
        hidden = []
        for half in range(2):
            inv_sqrt = scale((2 * part + half) * BLOCK, BLOCK)
            aggregated = summed(tile_col, tiles, columns_in, 2 * part + half, False)
            hidden.append(inv_sqrt * jnp.maximum(inv_sqrt * aggregated + bias_down, 0.0))
        hidden = jnp.concatenate(hidden, axis=1).astype(jnp.bfloat16)
        result = jnp.dot(w_outer[...], hidden, preferred_element_type=jnp.float32)
        spare = jnp.zeros((sum(sizes_out) - result.shape[0], CHUNK), jnp.float32)
        keep(outer, part, jnp.concatenate([result, spare], axis=0).astype(jnp.bfloat16))

    outer.start()
    outer.run()
    last_down = down(bias_outer[...])

    @pl.loop(0, SIDE)
    def _(part):
        for half in range(2):
            start = (2 * part + half) * BLOCK
            aggregated = jnp.transpose(summed(tile_col, tiles, columns_out, 2 * part + half, True))
            logits[:, pl.ds(start, BLOCK)] = scale(start, BLOCK) * aggregated[: logits.shape[0]] + last_down


def on_device(features, w_inner, bias_inner, w_outer, bias_outer, tiles, tile_col, degrees, send_rows):
    rows, _ = features.shape
    hidden = w_inner.shape[1]
    classes = w_outer.shape[1]
    sizes_in, sizes_out = (96, 80, 80), (16, 16, 16)
    send = send_rows.reshape(SIDE, SIDE, SIDE, CORES, BLOCK)
    vmem = pl.BlockSpec(memory_space=pltpu.VMEM)
    bf16 = jnp.bfloat16

    def held(sizes, chunk):
        return [pltpu.VMEM((CHIPS, rows // chunk * size, chunk), bf16) for size in sizes]

    def staged(sizes):
        return [pltpu.VMEM((PLANE, SIDE, size, BLOCK), bf16) for size in sizes]

    def columns(sizes):
        return pltpu.VMEM((SIDE + 1, SIDE, SIDE, CORES, sum(sizes), BLOCK), bf16)

    def sems():
        shapes = [(SIDE - 1,), (2, SIDE), (SIDE,), ()]
        return [pltpu.SemaphoreType.DMA((AXES, *shape)) for shape in shapes]

    return pl.pallas_call(
        functools.partial(kernel, sizes_in, sizes_out),
        out_shape=jax.ShapeDtypeStruct((classes, rows), jnp.float32),
        in_specs=[
            pl.BlockSpec(memory_space=pl.ANY),
            pl.BlockSpec(memory_space=pl.ANY),
            vmem,
            vmem,
            vmem,
            pl.BlockSpec(memory_space=pl.ANY),
            pl.BlockSpec(memory_space=pltpu.SMEM),
            vmem,
            vmem,
        ],
        out_specs=vmem,
        scratch_shapes=[
            pltpu.VMEM(tiles.shape, bf16),
            pltpu.SemaphoreType.DMA,
            pltpu.VMEM((AXES, SIDE, SIDE, SIDE, CORES, BLOCK), jnp.int32),
            pltpu.VMEM((AXES, SIDE, SIDE, SIDE, CORES, BLOCK), jnp.int32),
            *held(sizes_in, CHUNK),
            *staged(sizes_in),
            *held(sizes_out, BLOCK),
            *staged(sizes_out),
            columns(sizes_in),
            columns(sizes_out),
            pltpu.VMEM((features.shape[1], rows), bf16),
            pltpu.VMEM(w_inner.shape, bf16),
            pltpu.SemaphoreType.DMA((2,)),
            pltpu.SemaphoreType.DMA((2, AXES)),
            pltpu.SemaphoreType.DMA((2, AXES)),
            pltpu.SemaphoreType.DMA((AXES,)),
            pltpu.SemaphoreType.DMA((AXES,)),
            *sems(),
            *sems(),
            pltpu.VMEM((CHIPS, AXES, SIDE, BLOCK, 2 * BLOCK), bf16),
        ],
        compiler_params=pltpu.CompilerParams(
            collective_id=0, has_side_effects=True, vmem_limit_bytes=VMEM_LIMIT
        ),
    )(
        features.T,
        w_inner,
        bias_inner.reshape(1, hidden),
        w_outer.T,
        bias_outer.reshape(1, classes),
        tiles,
        tile_col,
        degrees.reshape(1, rows),
        send,
    ).T


def solution(mesh):
    return jax.shard_map(
        on_device,
        mesh=mesh,
        in_specs=(
            P(("dom", "sub"), None),
            P(),
            P(),
            P(),
            P(),
            P(("dom", "sub"), None, None, None),
            P(("dom", "sub"), None),
            P(("dom", "sub")),
            P(("dom", "sub"), None, None),
        ),
        out_specs=P(("dom", "sub"), None),
        check_vma=False,
    )
```
